512 devices in a mesh: grp: 8 (over z), row: 64 (over y, x, core).
Axes of the slice: x: 4, y: 8, z: 8, core: 2. Of those that a mesh axis runs over, the one named last changes fastest.
Arguments:
- tiles: bfloat16 [3072, 512, 512], P(('grp', 'row')), may hold values from -0.15625 to 0.15625
- tile_row: int32 [3072], P(('grp', 'row')), may hold values from 0 to 1023, as said below
- tile_col: int32 [3072], P(('grp', 'row')), may hold values from 0 to 1023, as said below
- tile_count: int32 [512], P(('grp', 'row')), may hold values from 3 to 6, as said below
- q_block: bfloat16 [524288, 256], P(('grp', 'row')), may hold values from -80 to 80
Outputs:
- q_next: float32 [524288, 256], P(('grp', 'row'))
The draws below stay inside these ranges and needn't reach their ends.
Inputs may be any that keep to these rules, and one draw needn't show every extreme that they name: `tile_row`: each slot names one of its device's tile rows: d * 2 to d * 2 + 1 for device d. `tile_col`: each slot's tile column is (tile_row + o) mod 1024 with o from minus 2 to 2; no two slots of one device name the same pair of tile row and tile column. `tile_count`: some device has all 6 slots live.
All inputs are finite; a program needn't handle non-finite values.
Results may differ from the reference program's by a relative error of at most 0.0029.
Values may be sent and summed in bfloat16 or wider, within the bound.
A program may use at most 64 MiB of HBM per device.

```python
import jax
import jax.numpy as jnp
from jax import lax

BS = 512
K = 256
TR = 2
H = 2
TILES_DEV = 6
NT = 1024
N = 524288
N_GRP = 8
N_ROW = 64


def slot_pairs(key):
    device_total = N_GRP * N_ROW
    span = 2 * H + 1
    pair_total = TR * span
    keys = jax.random.split(jax.random.fold_in(key, 31), device_total)
    scores = jax.vmap(lambda single: jax.random.permutation(single, pair_total))(keys).astype(jnp.int32)
    pair_ids = jnp.arange(pair_total, dtype=jnp.int32)[None, :]
    first_pair = H - 1
    second_pair = (TR - 1) * span + H + 1
    third_pair = H
    scores = jnp.where(pair_ids == first_pair, -3, jnp.where(pair_ids == second_pair, -2, jnp.where(pair_ids == third_pair, -1, scores)))
    order = jnp.argsort(scores, axis=1, stable=True)[:, :TILES_DEV].astype(jnp.int32)
    local_row = order // span
    offset = order % span - H
    device = jnp.arange(device_total, dtype=jnp.int32)[:, None]
    rows = device * TR + local_row
    cols = (rows + offset) % (TR * device_total)
    return (rows.reshape(-1).astype(jnp.int32), cols.reshape(-1).astype(jnp.int32))


def draw_tile_row(key, part):
    rows, cols = slot_pairs(key)
    return rows


def draw_tile_col(key, part):
    rows, cols = slot_pairs(key)
    return cols


def draw_tile_count(key, part):
    device_total = N_GRP * N_ROW
    counts = jax.random.randint(jax.random.fold_in(key, 21), (device_total,), 3, TILES_DEV + 1, dtype=jnp.int32)
    busiest = jax.random.randint(jax.random.fold_in(key, 22), (), 0, device_total, dtype=jnp.int32)
    device_ids = jnp.arange(device_total, dtype=jnp.int32)
    return jnp.where(device_ids == busiest, TILES_DEV, counts).astype(jnp.int32)


def draw_q_block(key, part):
    row_tile = jnp.arange(N, dtype=jnp.int32) // BS
    row_scale = 10.0 ** (row_tile.astype(jnp.float32) / (NT - 1))
    base = jnp.clip(jax.random.normal(jax.random.fold_in(key, 43), (N, K), jnp.float32), -6.0, 6.0)
    return (base * row_scale[:, None]).astype(jnp.bfloat16)


def steps_of(stream_key, dims, cuts, low, high):
    level = 1.0
    for position, shards_of in cuts:
        draws = jax.random.uniform(jax.random.fold_in(jax.random.fold_in(stream_key, 6), position), (shards_of,), jnp.float32, low / len(cuts), high / len(cuts))
        level = level * jnp.repeat(jnp.exp(draws), dims[position] // shards_of).reshape((-1,) + (1,) * (len(dims) - 1 - position))
    return level


def centred(rng, shape, deviation, reach, cuts=(), held_as=jnp.bfloat16):
    gain = steps_of(rng, shape, cuts, -0.22, 0.18) if cuts else 1.0
    array = jax.random.normal(rng, shape, jnp.float32) * deviation * gain
    return jnp.minimum(jnp.maximum(array, -reach), reach).astype(held_as)


def setup_inputs(seed: int = 0) -> dict:
    key_of = jax.random.split(jax.random.key(seed), 6)
    tiles = centred(key_of[0], (N_GRP * N_ROW * TILES_DEV, BS, BS), (BS * TILES_DEV // TR) ** -0.5, 0.15625, ((0, 512),))
    tile_row = draw_tile_row(jax.random.fold_in(key_of[5], 71), 0)
    tile_col = draw_tile_col(jax.random.fold_in(key_of[5], 71), 0)
    tile_count = draw_tile_count(jax.random.fold_in(key_of[5], 71), 0)
    q_block = draw_q_block(jax.random.fold_in(key_of[5], 71), 0)
    return dict(tiles=tiles, tile_row=tile_row, tile_col=tile_col, tile_count=tile_count, q_block=q_block)


def reference(tiles, tile_row, tile_col, tile_count, q_block):
    device_total = N_GRP * N_ROW
    tile_sets = tiles.reshape(device_total, TILES_DEV, BS, BS)
    slot_rows = tile_row.reshape(device_total, TILES_DEV)
    slot_cols = tile_col.reshape(device_total, TILES_DEV)
    q_tiles = q_block.astype(jnp.float32).reshape(NT, BS, K)
    slot_ids = jnp.arange(TILES_DEV, dtype=jnp.int32)
    row_ids = jnp.arange(TR, dtype=jnp.int32)
    column_ids = jnp.arange(TR + 2 * H, dtype=jnp.int32)

    def forward(device):
        live_slot = slot_ids < tile_count[device]
        local_row = (slot_rows[device] - device * TR).astype(jnp.int32)
        blocks = q_tiles[slot_cols[device]]
        products = jnp.einsum('sab,sbk->sak', tile_sets[device].astype(jnp.float32), blocks, precision=lax.Precision.HIGHEST)
        placing = ((local_row[None, :] == row_ids[:, None]) & live_slot[None, :]).astype(jnp.float32)
        return jnp.einsum('rs,sak->rak', placing, products, precision=lax.Precision.HIGHEST)
    aq_tiles = lax.map(forward, jnp.arange(device_total, dtype=jnp.int32)).reshape(NT, BS, K).astype(jnp.bfloat16)

    def backward(device):
        live_slot = slot_ids < tile_count[device]
        local_col = ((slot_cols[device] - device * TR + H) % NT).astype(jnp.int32)
        row_part = aq_tiles[slot_rows[device]].astype(jnp.float32)
        images = jnp.einsum('sab,sak->sbk', tile_sets[device].astype(jnp.float32), row_part, precision=lax.Precision.HIGHEST)
        placing = ((local_col[None, :] == column_ids[:, None]) & live_slot[None, :]).astype(jnp.float32)
        sums = jnp.einsum('cs,sbk->cbk', placing, images, precision=lax.Precision.HIGHEST)
        return (sums[H:H + TR], sums[:H].astype(jnp.bfloat16), sums[H + TR:].astype(jnp.bfloat16))
    own_part, lower, upper = lax.map(backward, jnp.arange(device_total, dtype=jnp.int32))
    lower, upper = lax.optimization_barrier((lower, upper))
    from_above = jnp.roll(lower, -1, axis=0).astype(jnp.float32)
    from_below = jnp.roll(upper, 1, axis=0).astype(jnp.float32)
    own_part = own_part.at[:, TR - H:].add(from_above)
    own_part = own_part.at[:, :H].add(from_below)
    y_full = own_part.reshape(N, K)
    gram_matrix = jnp.dot(y_full.T.astype(jnp.float32), y_full.astype(jnp.float32), precision=lax.Precision.HIGHEST, preferred_element_type=jnp.float32) / N
    factor_low = jnp.linalg.cholesky(gram_matrix)
    return lax.linalg.triangular_solve(factor_low, y_full, left_side=False, lower=True, transpose_a=True)
```

```python
import functools

import jax
import jax.numpy as jnp
from jax import lax
from jax.experimental import pallas as pl
from jax.experimental.pallas import tpu as pltpu
from jax.sharding import Mesh
from jax.sharding import PartitionSpec as P

H = 2
AXES = ("z", "y", "x", "c")
BF16 = jnp.bfloat16
F32 = jnp.float32


def dot(a, b, dims):
    return lax.dot_general(a, b, (dims, ((), ())), preferred_element_type=F32)


NN = ((1,), (0,))
TN = ((0,), (0,))


def step_kernel(
    sizes,
    row_ref, col_ref, count_ref, tiles_hbm, q_hbm,
    y_hbm, gram_ref,
    tiles, q_own, q_left, q_right, aq_acc, aq, rim_low, rim_high, got_left, got_right, y_own,
    terms, rs_in, st_out, s2_in, s3_in, piece,
    load_sem, y_sem, halo_send, halo_recv, rim_send, rim_recv,
    rs_send, rs_recv, s2_send, s2_recv, s3_send, s3_recv, ag_send, ag_recv,
):
    nz, ny, nx, nc = sizes
    bs = tiles.shape[1]
    z, y, x, c = (lax.axis_index(a) for a in AXES)
    me = ((z * ny + y) * nx + x) * nc + c
    total = nz * ny * nx * nc

    def coords(d):
        return (d // (ny * nx * nc), d // (nx * nc) % ny, d // nc % nx, d % nc)

    right, left = coords((me + 1) % total), coords((me + total - 1) % total)
    group = nx * nc
    mine = x * nc + c
    near = []
    for k in range(1, group):
        p = (mine + k) % group
        near.append((p, (z, y, p // nc, p % nc)))
    second = [(z, (y + k) % ny, x, c) for k in range(1, ny)]
    third = [((z + k) % nz, y, x, c) for k in range(1, nz)]
    assert ny == nz
    first_hop, second_hop = [], []
    for k in range(1, ny):
        first_hop.append(((z + k * c) % nz, (y + k * (1 - c)) % ny, x, c))
        second_hop.append(((z + k * (1 - c)) % nz, (y + k * c) % ny, x, c))
    at_first = y * (1 - c) + z * c
    at_second = z * (1 - c) + y * c

    q_load = pltpu.make_async_copy(q_hbm, q_own, load_sem.at[0])
    q_load.start()
    tile_load = pltpu.make_async_copy(tiles_hbm, tiles, load_sem.at[1])
    tile_load.start()

    barrier = pltpu.get_barrier_semaphore()
    peers = [left, right] + [d for _, d in near] + second + third
    for d in peers:
        pl.semaphore_signal(barrier, inc=1, device_id=d, device_id_type=pl.DeviceIdType.MESH)

    slot_count = tiles.shape[0]
    slot, held = {}, {}
    local_row = [row_ref[s] % 2 for s in range(slot_count)]
    offset = [(col_ref[s] - row_ref[s] + H + 2 * total) % (2 * total) for s in range(slot_count)]
    for r in range(2):
        for o in range(2 * H + 1):
            at, live = jnp.int32(0), jnp.int32(0)
            for s in range(slot_count):
                hit = (local_row[s] == r) & (offset[s] == o) & (s < count_ref[0])
                at = jnp.where(hit, s, at)
                live = jnp.where(hit, 1, live)
            slot[r, o], held[r, o] = at, live > 0

    pl.semaphore_wait(barrier, len(peers))
    q_load.wait()

    def send(src, dst, ssem, rsem, device):
        copy = pltpu.make_async_remote_copy(
            src_ref=src, dst_ref=dst, send_sem=ssem, recv_sem=rsem,
            device_id=device, device_id_type=pl.DeviceIdType.MESH,
        )
        copy.start()
        return copy

    to_left = send(q_own, q_right, halo_send.at[0], halo_recv.at[0], left)
    to_right = send(q_own, q_left, halo_send.at[1], halo_recv.at[1], right)
    tile_load.wait()

    def masked(block, r, o):
        return jnp.where(held[r, o], block, jnp.zeros_like(block))

    def forward(r, o, source, at):
        return dot(tiles[slot[r, o]], masked(source[pl.ds(at * bs, bs), :], r, o), NN)

    for r in range(2):
        aq_acc[r] = forward(r, H - r, q_own, 0) + forward(r, H - r + 1, q_own, 1)
    to_right.wait_recv()
    aq_acc[0] = aq_acc[0] + forward(0, 0, q_left, 0) + forward(0, 1, q_left, 1)
    aq_acc[1] = aq_acc[1] + forward(1, 0, q_left, 1)
    to_left.wait_recv()
    aq[0] = (aq_acc[0] + forward(0, 4, q_right, 0)).astype(BF16)
    aq[1] = (aq_acc[1] + forward(1, 3, q_right, 0) + forward(1, 4, q_right, 1)).astype(BF16)

    def backward(r, o):
        return dot(tiles[slot[r, o]], masked(aq[r], r, o), TN)

    low, high = pl.ds(0, bs), pl.ds(bs, bs)
    rim_low[low, :] = backward(0, 0).astype(BF16)
    rim_low[high, :] = (backward(0, 1) + backward(1, 0)).astype(BF16)
    rim_to_left = send(rim_low, got_right, rim_send.at[0], rim_recv.at[0], left)
    rim_high[low, :] = (backward(0, 4) + backward(1, 3)).astype(BF16)
    rim_high[high, :] = backward(1, 4).astype(BF16)
    rim_to_right = send(rim_high, got_left, rim_send.at[1], rim_recv.at[1], right)
    y_own[low, :] = backward(0, 2) + backward(1, 1)
    y_own[high, :] = backward(0, 3) + backward(1, 2)
    rim_to_right.wait_recv()
    rim_to_left.wait_recv()
    whole = y_own[...] + got_left[...].astype(F32) + got_right[...].astype(F32)
    y_own[...] = whole
    y_store = pltpu.make_async_copy(y_own, y_hbm, y_sem)
    y_store.start()
    big = whole.astype(BF16)
    small = (whole - big.astype(F32)).astype(BF16)
    local_gram = dot(big, big, TN) + dot(big, small, TN) + dot(small, big, TN)
    half = local_gram.shape[0] // 2
    rows = 3 * half // group
    terms[0 : half, :] = local_gram[:half, :half].astype(BF16)
    terms[half : 2 * half, :] = local_gram[half:, :half].astype(BF16)
    terms[2 * half :, :] = local_gram[half:, half:].astype(BF16)

    def part(p):
        return pl.ds(pl.multiple_of(p * rows, 16), rows)

    copies = []
    for k, (p, device) in enumerate(near):
        copies.append(
            send(terms.at[part(p), :], rs_in.at[mine], rs_send.at[k], rs_recv.at[k], device)
        )
    rs_in[mine] = terms[part(mine), :]
    for copy in copies:
        copy.wait_recv()
    acc = rs_in[0].astype(F32)
    for p in range(1, group):
        acc = acc + rs_in[p].astype(F32)
    st_out[0] = acc.astype(BF16)
    s2_in[at_first] = acc.astype(BF16)
    hop1 = []
    for k, device in enumerate(first_hop):
        hop1.append(
            send(st_out.at[0], s2_in.at[at_first], s2_send.at[k], s2_recv.at[k], device)
        )
    for copy in hop1:
        copy.wait_recv()
    acc = s2_in[0].astype(F32)
    for p in range(1, ny):
        acc = acc + s2_in[p].astype(F32)
    st_out[1] = acc.astype(BF16)
    s3_in[at_second] = acc.astype(BF16)
    hop2 = []
    for k, device in enumerate(second_hop):
        hop2.append(
            send(st_out.at[1], s3_in.at[at_second], s3_send.at[k], s3_recv.at[k], device)
        )
    for copy in hop2:
        copy.wait_recv()
    acc = s3_in[0].astype(F32)
    for p in range(1, nz):
        acc = acc + s3_in[p].astype(F32)
    piece[...] = acc.astype(BF16)
    gram_ref[part(mine), :] = acc.astype(BF16)
    out = []
    for k, (p, device) in enumerate(near):
        out.append(
            send(piece, gram_ref.at[part(mine), :], ag_send.at[k], ag_recv.at[k], device)
        )
    for copy in out:
        copy.wait_recv()
    y_store.wait()
    for copy in [to_left, to_right, rim_to_left, rim_to_right] + copies + hop1 + hop2 + out:
        copy.wait_send()


def summed_step(sizes, tiles, tile_row, tile_col, tile_count, q_block):
    slots, bs, _ = tiles.shape
    rows, width = q_block.shape
    half = width // 2
    nz, ny, nx, nc = sizes
    group = nx * nc
    part = 3 * half // group
    dma = pltpu.SemaphoreType.DMA
    smem = pl.BlockSpec(memory_space=pltpu.SMEM)
    anywhere = pl.BlockSpec(memory_space=pl.ANY)
    return pl.pallas_call(
        functools.partial(step_kernel, sizes),
        out_shape=(
            jax.ShapeDtypeStruct((rows, width), F32),
            jax.ShapeDtypeStruct((3 * half, half), BF16),
        ),
        in_specs=[smem, smem, smem, anywhere, anywhere],
        out_specs=(anywhere, pl.BlockSpec(memory_space=pltpu.VMEM)),
        scratch_shapes=[
            pltpu.VMEM((slots, bs, bs), BF16),
            pltpu.VMEM((rows, width), BF16),
            pltpu.VMEM((rows, width), BF16),
            pltpu.VMEM((rows, width), BF16),
            pltpu.VMEM((2, bs, width), F32),
            pltpu.VMEM((2, bs, width), BF16),
            pltpu.VMEM((rows, width), BF16),
            pltpu.VMEM((rows, width), BF16),
            pltpu.VMEM((rows, width), BF16),
            pltpu.VMEM((rows, width), BF16),
            pltpu.VMEM((rows, width), F32),
            pltpu.VMEM((3 * half, half), BF16),
            pltpu.VMEM((group, part, half), BF16),
            pltpu.VMEM((2, part, half), BF16),
            pltpu.VMEM((ny, part, half), BF16),
            pltpu.VMEM((nz, part, half), BF16),
            pltpu.VMEM((part, half), BF16),
            dma((2,)), dma, dma((2,)), dma((2,)), dma((2,)), dma((2,)),
            dma((group - 1,)), dma((group - 1,)), dma((ny - 1,)), dma((ny - 1,)),
            dma((nz - 1,)), dma((nz - 1,)), dma((group - 1,)), dma((group - 1,)),
        ],
        compiler_params=pltpu.CompilerParams(
            collective_id=0, has_side_effects=True, vmem_limit_bytes=40 * 1024 * 1024
        ),
        name="step",
    )(tile_row, tile_col, tile_count, tiles, q_block)


def on_device(sizes, tiles, tile_row, tile_col, tile_count, q_block):
    local_y, packed = summed_step(sizes, tiles, tile_row, tile_col, tile_count, q_block)
    half = packed.shape[1]
    blocks = packed.astype(F32)
    corner = blocks[half : 2 * half]
    gram = jnp.concatenate(
        [
            jnp.concatenate([blocks[:half], corner.T], axis=1),
            jnp.concatenate([corner, blocks[2 * half :]], axis=1),
        ],
        axis=0,
    )
    rows_total = local_y.shape[0] * sizes[0] * sizes[1] * sizes[2] * sizes[3]
    factor_low = jnp.linalg.cholesky(gram / rows_total)
    return lax.linalg.triangular_solve(
        factor_low, local_y, left_side=False, lower=True, transpose_a=True
    )


def solution(mesh):
    nz = mesh.shape["grp"]
    sizes = (nz, 8, mesh.shape["row"] // 16, 2)
    torus = Mesh(mesh.devices.reshape(sizes), AXES)
    return jax.shard_map(
        functools.partial(on_device, sizes),
        mesh=torus,
        in_specs=(P(AXES, None, None), P(AXES), P(AXES), P(AXES), P(AXES, None)),
        out_specs=P(AXES, None),
        check_vma=False,
    )
```

```python
import functools

import jax
import jax.numpy as jnp
from jax import lax
from jax.experimental import pallas as pl
from jax.experimental.pallas import tpu as pltpu
from jax.sharding import Mesh
from jax.sharding import PartitionSpec as P

H = 2
AXES = ("z", "y", "x", "c")
BF16 = jnp.bfloat16
F32 = jnp.float32


def dot(a, b, dims):
    return lax.dot_general(a, b, (dims, ((), ())), preferred_element_type=F32)


NN = ((1,), (0,))
TN = ((0,), (0,))
NT = ((1,), (1,))


def step_kernel(
    sizes,
    row_ref, col_ref, count_ref, tiles_hbm, q_hbm,
    big_hbm, small_hbm, gram_ref,
    tiles, q_own, q_left, q_right, aq_acc, aq, rim_low, rim_high, got_left, got_right, y_own, y_big, y_small,
    terms, rs_in, st_out, s2_in, s3_in, piece,
    load_sem, y_sem, halo_send, halo_recv, rim_send, rim_recv,
    rs_send, rs_recv, s2_send, s2_recv, s3_send, s3_recv, ag_send, ag_recv,
):
    nz, ny, nx, nc = sizes
    bs = tiles.shape[1]
    z, y, x, c = (lax.axis_index(a) for a in AXES)
    me = ((z * ny + y) * nx + x) * nc + c
    total = nz * ny * nx * nc

    def coords(d):
        return (d // (ny * nx * nc), d // (nx * nc) % ny, d // nc % nx, d % nc)

    right, left = coords((me + 1) % total), coords((me + total - 1) % total)
    group = nx * nc
    mine = x * nc + c
    near = []
    for k in range(1, group):
        p = (mine + k) % group
        near.append((p, (z, y, p // nc, p % nc)))
    second = [(z, (y + k) % ny, x, c) for k in range(1, ny)]
    third = [((z + k) % nz, y, x, c) for k in range(1, nz)]
    assert ny == nz
    first_hop, second_hop = [], []
    for k in range(1, ny):
        first_hop.append(((z + k * c) % nz, (y + k * (1 - c)) % ny, x, c))
        second_hop.append(((z + k * (1 - c)) % nz, (y + k * c) % ny, x, c))
    at_first = y * (1 - c) + z * c
    at_second = z * (1 - c) + y * c

    q_load = pltpu.make_async_copy(q_hbm, q_own, load_sem.at[0])
    q_load.start()
    tile_load = pltpu.make_async_copy(tiles_hbm, tiles, load_sem.at[1])
    tile_load.start()

    barrier = pltpu.get_barrier_semaphore()
    peers = [left, right] + [d for _, d in near] + second + third
    for d in peers:
        pl.semaphore_signal(barrier, inc=1, device_id=d, device_id_type=pl.DeviceIdType.MESH)

    slot_count = tiles.shape[0]
    slot, held = {}, {}
    local_row = [row_ref[s] % 2 for s in range(slot_count)]
    offset = [(col_ref[s] - row_ref[s] + H + 2 * total) % (2 * total) for s in range(slot_count)]
    for r in range(2):
        for o in range(2 * H + 1):
            at, live = jnp.int32(0), jnp.int32(0)
            for s in range(slot_count):
                hit = (local_row[s] == r) & (offset[s] == o) & (s < count_ref[0])
                at = jnp.where(hit, s, at)
                live = jnp.where(hit, 1, live)
            slot[r, o], held[r, o] = at, live > 0

    pl.semaphore_wait(barrier, len(peers))
    q_load.wait()

    def send(src, dst, ssem, rsem, device):
        copy = pltpu.make_async_remote_copy(
            src_ref=src, dst_ref=dst, send_sem=ssem, recv_sem=rsem,
            device_id=device, device_id_type=pl.DeviceIdType.MESH,
        )
        copy.start()
        return copy

    to_left = send(q_own, q_right, halo_send.at[0], halo_recv.at[0], left)
    to_right = send(q_own, q_left, halo_send.at[1], halo_recv.at[1], right)
    tile_load.wait()

    def masked(block, r, o):
        return jnp.where(held[r, o], block, jnp.zeros_like(block))

    def forward(r, o, source, at):
        return dot(tiles[slot[r, o]], masked(source[pl.ds(at * bs, bs), :], r, o), NN)

    for r in range(2):
        aq_acc[r] = forward(r, H - r, q_own, 0) + forward(r, H - r + 1, q_own, 1)
    to_right.wait_recv()
    aq_acc[0] = aq_acc[0] + forward(0, 0, q_left, 0) + forward(0, 1, q_left, 1)
    aq_acc[1] = aq_acc[1] + forward(1, 0, q_left, 1)
    to_left.wait_recv()
    aq[0] = (aq_acc[0] + forward(0, 4, q_right, 0)).astype(BF16)
    aq[1] = (aq_acc[1] + forward(1, 3, q_right, 0) + forward(1, 4, q_right, 1)).astype(BF16)

    def backward(r, o):
        return dot(tiles[slot[r, o]], masked(aq[r], r, o), TN)

    low, high = pl.ds(0, bs), pl.ds(bs, bs)
    rim_low[low, :] = backward(0, 0).astype(BF16)
    rim_low[high, :] = (backward(0, 1) + backward(1, 0)).astype(BF16)
    rim_to_left = send(rim_low, got_right, rim_send.at[0], rim_recv.at[0], left)
    rim_high[low, :] = (backward(0, 4) + backward(1, 3)).astype(BF16)
    rim_high[high, :] = backward(1, 4).astype(BF16)
    rim_to_right = send(rim_high, got_left, rim_send.at[1], rim_recv.at[1], right)
    y_own[low, :] = backward(0, 2) + backward(1, 1)
    y_own[high, :] = backward(0, 3) + backward(1, 2)
    rim_to_right.wait_recv()
    rim_to_left.wait_recv()
    whole = y_own[...] + got_left[...].astype(F32) + got_right[...].astype(F32)
    big = whole.astype(BF16)
    small = (whole - big.astype(F32)).astype(BF16)
    y_big[...] = big
    y_small[...] = small
    local_gram = dot(big, big, TN) + dot(big, small, TN) + dot(small, big, TN)
    half = local_gram.shape[0] // 2
    rows = 3 * half // group
    terms[0 : half, :] = local_gram[:half, :half].astype(BF16)
    terms[half : 2 * half, :] = local_gram[half:, :half].astype(BF16)
    terms[2 * half :, :] = local_gram[half:, half:].astype(BF16)
    stores = [
        pltpu.make_async_copy(y_big, big_hbm, y_sem.at[0]),
        pltpu.make_async_copy(y_small, small_hbm, y_sem.at[1]),
    ]

    def part(p):
        return pl.ds(pl.multiple_of(p * rows, 16), rows)

    copies = []
    for k, (p, device) in enumerate(near):
        copies.append(
            send(terms.at[part(p), :], rs_in.at[mine], rs_send.at[k], rs_recv.at[k], device)
        )
    rs_in[mine] = terms[part(mine), :]
    for store in stores:
        store.start()
    for copy in copies:
        copy.wait_recv()
    acc = rs_in[0].astype(F32)
    for p in range(1, group):
        acc = acc + rs_in[p].astype(F32)
    st_out[0] = acc.astype(BF16)
    s2_in[at_first] = acc.astype(BF16)
    hop1 = []
    for k, device in enumerate(first_hop):
        hop1.append(
            send(st_out.at[0], s2_in.at[at_first], s2_send.at[k], s2_recv.at[k], device)
        )
    for copy in hop1:
        copy.wait_recv()
    acc = s2_in[0].astype(F32)
    for p in range(1, ny):
        acc = acc + s2_in[p].astype(F32)
    st_out[1] = acc.astype(BF16)
    s3_in[at_second] = acc.astype(BF16)
    hop2 = []
    for k, device in enumerate(second_hop):
        hop2.append(
            send(st_out.at[1], s3_in.at[at_second], s3_send.at[k], s3_recv.at[k], device)
        )
    for copy in hop2:
        copy.wait_recv()
    acc = s3_in[0].astype(F32)
    for p in range(1, nz):
        acc = acc + s3_in[p].astype(F32)
    piece[...] = acc.astype(BF16)
    gram_ref[part(mine), :] = acc.astype(BF16)
    out = []
    for k, (p, device) in enumerate(near):
        out.append(
            send(piece, gram_ref.at[part(mine), :], ag_send.at[k], ag_recv.at[k], device)
        )
    for copy in out:
        copy.wait_recv()
    for store in stores:
        store.wait()
    for copy in [to_left, to_right, rim_to_left, rim_to_right] + copies + hop1 + hop2 + out:
        copy.wait_send()


def summed_step(sizes, tiles, tile_row, tile_col, tile_count, q_block):
    slots, bs, _ = tiles.shape
    rows, width = q_block.shape
    half = width // 2
    nz, ny, nx, nc = sizes
    group = nx * nc
    part = 3 * half // group
    dma = pltpu.SemaphoreType.DMA
    smem = pl.BlockSpec(memory_space=pltpu.SMEM)
    anywhere = pl.BlockSpec(memory_space=pl.ANY)
    return pl.pallas_call(
        functools.partial(step_kernel, sizes),
        out_shape=(
            jax.ShapeDtypeStruct((rows, width), BF16),
            jax.ShapeDtypeStruct((rows, width), BF16),
            jax.ShapeDtypeStruct((3 * half, half), BF16),
        ),
        in_specs=[smem, smem, smem, anywhere, anywhere],
        out_specs=(anywhere, anywhere, pl.BlockSpec(memory_space=pltpu.VMEM)),
        scratch_shapes=[
            pltpu.VMEM((slots, bs, bs), BF16),
            pltpu.VMEM((rows, width), BF16),
            pltpu.VMEM((rows, width), BF16),
            pltpu.VMEM((rows, width), BF16),
            pltpu.VMEM((2, bs, width), F32),
            pltpu.VMEM((2, bs, width), BF16),
            pltpu.VMEM((rows, width), BF16),
            pltpu.VMEM((rows, width), BF16),
            pltpu.VMEM((rows, width), BF16),
            pltpu.VMEM((rows, width), BF16),
            pltpu.VMEM((rows, width), F32),
            pltpu.VMEM((rows, width), BF16),
            pltpu.VMEM((rows, width), BF16),
            pltpu.VMEM((3 * half, half), BF16),
            pltpu.VMEM((group, part, half), BF16),
            pltpu.VMEM((2, part, half), BF16),
            pltpu.VMEM((ny, part, half), BF16),
            pltpu.VMEM((nz, part, half), BF16),
            pltpu.VMEM((part, half), BF16),
            dma((2,)), dma((2,)), dma((2,)), dma((2,)), dma((2,)), dma((2,)),
            dma((group - 1,)), dma((group - 1,)), dma((ny - 1,)), dma((ny - 1,)),
            dma((nz - 1,)), dma((nz - 1,)), dma((group - 1,)), dma((group - 1,)),
        ],
        compiler_params=pltpu.CompilerParams(
            collective_id=0, has_side_effects=True, vmem_limit_bytes=40 * 1024 * 1024
        ),
        name="step",
    )(tile_row, tile_col, tile_count, tiles, q_block)


BLOCK = 32


def row_of(tile, s):
    return jnp.broadcast_to(tile[s : s + 1, :], tile.shape)


def eliminate(work, inverse, k):
    n = work.shape[0]
    start = BLOCK * k
    tiles, lane_tiles = BLOCK // 8, n // 128
    own, first = start // 128, start % 128
    sub = lax.broadcasted_iota(jnp.int32, (8, 128), 0)
    lane = lax.broadcasted_iota(jnp.int32, (8, 128), 1)
    inside = (lane >= first) & (lane < first + BLOCK)
    panel = [
        [work[start + 8 * i : start + 8 * i + 8, 128 * h : 128 * h + 128] for h in range(lane_tiles)]
        for i in range(tiles)
    ]
    column = {}
    for j in range(BLOCK):
        for i in range(j // 8, tiles):
            diagonal = panel[i][own]
            column[j, i] = jnp.broadcast_to(diagonal[:, first + j : first + j + 1], (8, 128))
    for i in range(tiles):
        unit = jnp.where(lane == sub + (first + 8 * i), 1.0, 0.0)
        panel[i][own] = jnp.where(inside, unit, panel[i][own])
    scale = [jnp.zeros((8, 128), F32) for _ in range(tiles)]
    for j in range(BLOCK):
        t, s = j // 8, j % 8
        root = lax.rsqrt(row_of(column[j, t], s))
        pivot = root * root
        scale[t] = jnp.where(sub == s, root, scale[t])
        factor = {i: column[j, i] * pivot for i in range(t, tiles)}
        factor[t] = jnp.where(sub > s, factor[t], 0.0)
        for k2 in range(j + 1, BLOCK):
            value = row_of(column[j, k2 // 8], k2 % 8)
            for i in range(k2 // 8, tiles):
                column[k2, i] = column[k2, i] - factor[i] * value
        for h in range(lane_tiles):
            value = row_of(panel[t][h], s)
            for i in range(t, tiles):
                panel[i][h] = panel[i][h] - factor[i] * value
    for i in range(tiles):
        for h in range(lane_tiles):
            panel[i][h] = panel[i][h] * scale[i]
            done = lane + 128 * h < start + BLOCK
            inverse[start + 8 * i : start + 8 * i + 8, 128 * h : 128 * h + 128] = jnp.where(
                done, panel[i][h], 0.0
            )
    rest = start + BLOCK
    if rest == n:
        return
    rows = jnp.concatenate([jnp.concatenate(p, axis=1) for p in panel], axis=0)
    big = rows.astype(BF16)
    small = (rows - big.astype(F32)).astype(BF16)
    base = 128 * (rest // 128)
    left = jnp.concatenate([big, big, small], axis=0)[:, base:]
    update = dot(left, jnp.concatenate([big, small, big], axis=0), TN)
    wide = lax.broadcasted_iota(jnp.int32, (n - rest, n), 1)
    kept = jnp.where((wide >= start) & (wide < rest), 0.0, work[rest:, :])
    work[rest:, :] = kept - update[rest - base :, :]


def solve_kernel(
    rows_total, gram_ref, big_hbm, small_hbm, out_hbm,
    y_big, y_small, work, inverse, out, load_sem, store_sem,
):
    loads = [
        pltpu.make_async_copy(big_hbm, y_big, load_sem.at[0]),
        pltpu.make_async_copy(small_hbm, y_small, load_sem.at[1]),
    ]
    for load in loads:
        load.start()
    n = work.shape[0]
    half = n // 2
    blocks = gram_ref[...].astype(F32) * (1.0 / rows_total)
    work[:half, :half] = blocks[:half]
    work[half:, :half] = blocks[half : 2 * half]
    work[:half, half:] = blocks[half : 2 * half].T
    work[half:, half:] = blocks[2 * half :]
    for k in range(n // BLOCK):
        eliminate(work, inverse, k)
    factor = inverse[...]
    big = factor.astype(BF16)
    small = (factor - big.astype(F32)).astype(BF16)
    for load in loads:
        load.wait()
    chunk = 256
    stores = []
    for i in range(y_big.shape[0] // chunk):
        span = pl.ds(i * chunk, chunk)
        out[span, :] = (
            dot(y_big[span, :], big, NT) + dot(y_big[span, :], small, NT) + dot(y_small[span, :], big, NT)
        )
        stores.append(pltpu.make_async_copy(out.at[span, :], out_hbm.at[span, :], store_sem.at[i]))
        stores[-1].start()
    for store in stores:
        store.wait()


def solved(rows_total, packed, y_big, y_small):
    rows, width = y_big.shape
    anywhere = pl.BlockSpec(memory_space=pl.ANY)
    dma = pltpu.SemaphoreType.DMA
    return pl.pallas_call(
        functools.partial(solve_kernel, rows_total),
        out_shape=jax.ShapeDtypeStruct((rows, width), F32),
        in_specs=[pl.BlockSpec(memory_space=pltpu.VMEM), anywhere, anywhere],
        out_specs=anywhere,
        scratch_shapes=[
            pltpu.VMEM((rows, width), BF16),
            pltpu.VMEM((rows, width), BF16),
            pltpu.VMEM((width, width), F32),
            pltpu.VMEM((width, width), F32),
            pltpu.VMEM((rows, width), F32),
            dma((2,)),
            dma((rows // 256,)),
        ],
        compiler_params=pltpu.CompilerParams(vmem_limit_bytes=24 * 1024 * 1024),
        name="solve",
    )(packed, y_big, y_small)


def on_device(sizes, tiles, tile_row, tile_col, tile_count, q_block):
    y_big, y_small, packed = summed_step(sizes, tiles, tile_row, tile_col, tile_count, q_block)
    rows_total = q_block.shape[0] * sizes[0] * sizes[1] * sizes[2] * sizes[3]
    return solved(rows_total, packed, y_big, y_small)


def solution(mesh):
    nz = mesh.shape["grp"]
    sizes = (nz, 8, mesh.shape["row"] // 16, 2)
    torus = Mesh(mesh.devices.reshape(sizes), AXES)
    return jax.shard_map(
        functools.partial(on_device, sizes),
        mesh=torus,
        in_specs=(P(AXES, None, None), P(AXES), P(AXES), P(AXES), P(AXES, None)),
        out_specs=P(AXES, None),
        check_vma=False,
    )
```

```python
import functools

import jax
import jax.numpy as jnp
from jax import lax
from jax.experimental import pallas as pl
from jax.experimental.pallas import tpu as pltpu
from jax.sharding import Mesh
from jax.sharding import PartitionSpec as P

H = 2
AXES = ("z", "y", "x", "c")
BF16 = jnp.bfloat16
F32 = jnp.float32


def dot(a, b, dims):
    return lax.dot_general(a, b, (dims, ((), ())), preferred_element_type=F32)


NN = ((1,), (0,))
TN = ((0,), (0,))
NT = ((1,), (1,))


def step_kernel(
    sizes,
    count_ref, row_hbm, col_hbm, tiles_hbm, q_hbm,
    y_big, y_small, gram_ref,
    row_ref, col_ref, tiles, q_own, q_left, q_right, aq_acc, aq, rim_low, rim_high, got_left, got_right, y_own,
    terms, rs_in, st_out, s2_in, s3_in, piece,
    load_sem, halo_send, halo_recv, rim_send, rim_recv,
    rs_send, rs_recv, s2_send, s2_recv, s3_send, s3_recv, ag_send, ag_recv,
):
    nz, ny, nx, nc = sizes
    bs = tiles.shape[1]
    z, y, x, c = (lax.axis_index(a) for a in AXES)
    me = ((z * ny + y) * nx + x) * nc + c
    total = nz * ny * nx * nc

    def coords(d):
        return (d // (ny * nx * nc), d // (nx * nc) % ny, d // nc % nx, d % nc)

    right, left = coords((me + 1) % total), coords((me + total - 1) % total)
    group = nx * nc
    mine = x * nc + c
    near = []
    for k in range(1, group):
        p = (mine + k) % group
        near.append((p, (z, y, p // nc, p % nc)))
    second = [(z, (y + k) % ny, x, c) for k in range(1, ny)]
    third = [((z + k) % nz, y, x, c) for k in range(1, nz)]
    assert ny == nz
    first_hop, second_hop = [], []
    for k in range(1, ny):
        first_hop.append(((z + k * c) % nz, (y + k * (1 - c)) % ny, x, c))
        second_hop.append(((z + k * (1 - c)) % nz, (y + k * c) % ny, x, c))
    at_first = y * (1 - c) + z * c
    at_second = z * (1 - c) + y * c

    index_loads = []
    for k, (src, dst) in enumerate(((row_hbm, row_ref), (col_hbm, col_ref))):
        index_loads.append(pltpu.make_async_copy(src, dst, load_sem.at[2 + k]))
        index_loads[-1].start()
    q_load = pltpu.make_async_copy(q_hbm, q_own, load_sem.at[0])
    q_load.start()
    tile_load = pltpu.make_async_copy(tiles_hbm, tiles, load_sem.at[1])
    tile_load.start()

    barrier = pltpu.get_barrier_semaphore()
    peers = [left, right] + [d for _, d in near] + second + third
    for d in peers:
        pl.semaphore_signal(barrier, inc=1, device_id=d, device_id_type=pl.DeviceIdType.MESH)

    for load in index_loads:
        load.wait()
    slot_count = tiles.shape[0]
    slot, held = {}, {}
    local_row = [row_ref[s] % 2 for s in range(slot_count)]
    offset = [(col_ref[s] - row_ref[s] + H + 2 * total) % (2 * total) for s in range(slot_count)]
    for r in range(2):
        for o in range(2 * H + 1):
            at, live = jnp.int32(0), jnp.int32(0)
            for s in range(slot_count):
                hit = (local_row[s] == r) & (offset[s] == o) & (s < count_ref[0])
                at = jnp.where(hit, s, at)
                live = jnp.where(hit, 1, live)
            slot[r, o], held[r, o] = at, live > 0

    pl.semaphore_wait(barrier, len(peers))
    q_load.wait()

    def send(src, dst, ssem, rsem, device):
        copy = pltpu.make_async_remote_copy(
            src_ref=src, dst_ref=dst, send_sem=ssem, recv_sem=rsem,
            device_id=device, device_id_type=pl.DeviceIdType.MESH,
        )
        copy.start()
        return copy

    to_left, to_right = [], []
    for k in range(2):
        tile = pl.ds(k * bs, bs)
        to_left.append(
            send(q_own.at[tile], q_right.at[tile], halo_send.at[k], halo_recv.at[k], left)
        )
        tile = pl.ds((1 - k) * bs, bs)
        to_right.append(
            send(q_own.at[tile], q_left.at[tile], halo_send.at[2 + k], halo_recv.at[2 + k], right)
        )
    tile_load.wait()

    def masked(block, r, o):
        return jnp.where(held[r, o], block, jnp.zeros_like(block))

    def forward(r, o, source, at):
        return dot(tiles[slot[r, o]], masked(source[pl.ds(at * bs, bs), :], r, o), NN)

    for r in range(2):
        aq_acc[r] = forward(r, H - r, q_own, 0) + forward(r, H - r + 1, q_own, 1)
    to_left[0].wait_recv()
    aq_acc[0] = aq_acc[0] + forward(0, 4, q_right, 0)
    aq_acc[1] = aq_acc[1] + forward(1, 3, q_right, 0)
    to_right[0].wait_recv()
    aq_acc[0] = aq_acc[0] + forward(0, 1, q_left, 1)
    aq_acc[1] = aq_acc[1] + forward(1, 0, q_left, 1)
    to_right[1].wait_recv()
    aq[0] = (aq_acc[0] + forward(0, 0, q_left, 0)).astype(BF16)
    to_left[1].wait_recv()
    aq[1] = (aq_acc[1] + forward(1, 4, q_right, 1)).astype(BF16)

    def backward(r, o):
        return dot(tiles[slot[r, o]], masked(aq[r], r, o), TN)

    low, high = pl.ds(0, bs), pl.ds(bs, bs)
    rim = []

    def send_rim(k, src, dst, span, device):
        rim.append(send(src.at[span], dst.at[span], rim_send.at[k], rim_recv.at[k], device))

    rim_low[low, :] = backward(0, 0).astype(BF16)
    send_rim(0, rim_low, got_right, low, left)
    rim_high[low, :] = (backward(0, 4) + backward(1, 3)).astype(BF16)
    send_rim(1, rim_high, got_left, low, right)
    rim_low[high, :] = (backward(0, 1) + backward(1, 0)).astype(BF16)
    send_rim(2, rim_low, got_right, high, left)
    rim_high[high, :] = backward(1, 4).astype(BF16)
    send_rim(3, rim_high, got_left, high, right)
    y_own[low, :] = backward(0, 2) + backward(1, 1)
    y_own[high, :] = backward(0, 3) + backward(1, 2)
    grams = []
    for k, span in enumerate((low, high)):
        rim[2 * k].wait_recv()
        rim[2 * k + 1].wait_recv()
        whole = y_own[span, :] + got_left[span, :].astype(F32) + got_right[span, :].astype(F32)
        big = whole.astype(BF16)
        small = (whole - big.astype(F32)).astype(BF16)
        y_big[span, :] = big
        y_small[span, :] = small
        grams.append(dot(big, big, TN) + dot(big, small, TN) + dot(small, big, TN))
    local_gram = grams[0] + grams[1]
    half = local_gram.shape[0] // 2
    rows = 3 * half // group
    terms[0 : half, :] = local_gram[:half, :half].astype(BF16)
    terms[half : 2 * half, :] = local_gram[half:, :half].astype(BF16)
    terms[2 * half :, :] = local_gram[half:, half:].astype(BF16)

    def part(p):
        return pl.ds(pl.multiple_of(p * rows, 16), rows)

    copies = []
    for k, (p, device) in enumerate(near):
        copies.append(
            send(terms.at[part(p), :], rs_in.at[mine], rs_send.at[k], rs_recv.at[k], device)
        )
    rs_in[mine] = terms[part(mine), :]
    for copy in copies:
        copy.wait_recv()
    acc = rs_in[0].astype(F32)
    for p in range(1, group):
        acc = acc + rs_in[p].astype(F32)
    st_out[0] = acc.astype(BF16)
    s2_in[at_first] = acc.astype(BF16)
    hop1 = []
    for k, device in enumerate(first_hop):
        hop1.append(
            send(st_out.at[0], s2_in.at[at_first], s2_send.at[k], s2_recv.at[k], device)
        )
    for copy in hop1:
        copy.wait_recv()
    acc = s2_in[0].astype(F32)
    for p in range(1, ny):
        acc = acc + s2_in[p].astype(F32)
    st_out[1] = acc.astype(BF16)
    s3_in[at_second] = acc.astype(BF16)
    hop2 = []
    for k, device in enumerate(second_hop):
        hop2.append(
            send(st_out.at[1], s3_in.at[at_second], s3_send.at[k], s3_recv.at[k], device)
        )
    for copy in hop2:
        copy.wait_recv()
    acc = s3_in[0].astype(F32)
    for p in range(1, nz):
        acc = acc + s3_in[p].astype(F32)
    piece[...] = acc.astype(BF16)
    gram_ref[part(mine), :] = acc.astype(BF16)
    out = []
    for k, (p, device) in enumerate(near):
        out.append(
            send(piece, gram_ref.at[part(mine), :], ag_send.at[k], ag_recv.at[k], device)
        )
    for copy in out:
        copy.wait_recv()
    for copy in to_left + to_right + rim + copies + hop1 + hop2 + out:
        copy.wait_send()


def summed_step(sizes, tiles, tile_row, tile_col, tile_count, q_block):
    slots, bs, _ = tiles.shape
    rows, width = q_block.shape
    half = width // 2
    nz, ny, nx, nc = sizes
    group = nx * nc
    part = 3 * half // group
    dma = pltpu.SemaphoreType.DMA
    hbm = pl.BlockSpec(memory_space=pltpu.HBM)
    vmem = pl.BlockSpec(memory_space=pltpu.VMEM)
    return pl.pallas_call(
        functools.partial(step_kernel, sizes),
        out_shape=(
            jax.ShapeDtypeStruct((rows, width), BF16),
            jax.ShapeDtypeStruct((rows, width), BF16),
            jax.ShapeDtypeStruct((3 * half, half), BF16),
        ),
        in_specs=[pl.BlockSpec(memory_space=pltpu.SMEM)] + [hbm] * 4,
        out_specs=(vmem, vmem, vmem),
        scratch_shapes=[
            pltpu.SMEM(tile_row.shape, jnp.int32),
            pltpu.SMEM(tile_col.shape, jnp.int32),
            pltpu.VMEM((slots, bs, bs), BF16),
            pltpu.VMEM((rows, width), BF16),
            pltpu.VMEM((rows, width), BF16),
            pltpu.VMEM((rows, width), BF16),
            pltpu.VMEM((2, bs, width), F32),
            pltpu.VMEM((2, bs, width), BF16),
            pltpu.VMEM((rows, width), BF16),
            pltpu.VMEM((rows, width), BF16),
            pltpu.VMEM((rows, width), BF16),
            pltpu.VMEM((rows, width), BF16),
            pltpu.VMEM((rows, width), F32),
            pltpu.VMEM((3 * half, half), BF16),
            pltpu.VMEM((group, part, half), BF16),
            pltpu.VMEM((2, part, half), BF16),
            pltpu.VMEM((ny, part, half), BF16),
            pltpu.VMEM((nz, part, half), BF16),
            pltpu.VMEM((part, half), BF16),
            dma((4,)), dma((4,)), dma((4,)), dma((4,)), dma((4,)),
            dma((group - 1,)), dma((group - 1,)), dma((ny - 1,)), dma((ny - 1,)),
            dma((nz - 1,)), dma((nz - 1,)), dma((group - 1,)), dma((group - 1,)),
        ],
        compiler_params=pltpu.CompilerParams(
            collective_id=0, has_side_effects=True, vmem_limit_bytes=40 * 1024 * 1024
        ),
        name="step",
    )(
        tile_count,
        *(
            pltpu.with_memory_space_constraint(a, pltpu.HBM)
            for a in (tile_row, tile_col, tiles, q_block)
        ),
    )


BLOCK = 32


def row_of(tile, s):
    return jnp.broadcast_to(tile[s : s + 1, :], tile.shape)


def eliminate(work, inverse, k):
    n = work.shape[0]
    start = BLOCK * k
    tiles, lane_tiles = BLOCK // 8, n // 128
    own, first = start // 128, start % 128
    sub = lax.broadcasted_iota(jnp.int32, (8, 128), 0)
    lane = lax.broadcasted_iota(jnp.int32, (8, 128), 1)
    inside = (lane >= first) & (lane < first + BLOCK)
    panel = [
        [work[start + 8 * i : start + 8 * i + 8, 128 * h : 128 * h + 128] for h in range(lane_tiles)]
        for i in range(tiles)
    ]
    column = {}
    for j in range(BLOCK):
        for i in range(j // 8, tiles):
            diagonal = panel[i][own]
            column[j, i] = jnp.broadcast_to(diagonal[:, first + j : first + j + 1], (8, 128))
    for i in range(tiles):
        unit = jnp.where(lane == sub + (first + 8 * i), 1.0, 0.0)
        panel[i][own] = jnp.where(inside, unit, panel[i][own])
    scale = [jnp.zeros((8, 128), F32) for _ in range(tiles)]
    for j in range(BLOCK):
        t, s = j // 8, j % 8
        root = lax.rsqrt(row_of(column[j, t], s))
        pivot = root * root
        scale[t] = jnp.where(sub == s, root, scale[t])
        factor = {i: column[j, i] * pivot for i in range(t, tiles)}
        factor[t] = jnp.where(sub > s, factor[t], 0.0)
        for k2 in range(j + 1, BLOCK):
            value = row_of(column[j, k2 // 8], k2 % 8)
            for i in range(k2 // 8, tiles):
                column[k2, i] = column[k2, i] - factor[i] * value
        for h in range(lane_tiles):
            value = row_of(panel[t][h], s)
            for i in range(t, tiles):
                panel[i][h] = panel[i][h] - factor[i] * value
    for i in range(tiles):
        for h in range(lane_tiles):
            panel[i][h] = panel[i][h] * scale[i]
            done = lane + 128 * h < start + BLOCK
            inverse[start + 8 * i : start + 8 * i + 8, 128 * h : 128 * h + 128] = jnp.where(
                done, panel[i][h], 0.0
            )
    rest = start + BLOCK
    if rest == n:
        return
    rows = jnp.concatenate([jnp.concatenate(p, axis=1) for p in panel], axis=0)
    big = rows.astype(BF16)
    small = (rows - big.astype(F32)).astype(BF16)
    base = 128 * (rest // 128)
    left = jnp.concatenate([big, big, small], axis=0)[:, base:]
    update = dot(left, jnp.concatenate([big, small, big], axis=0), TN)
    wide = lax.broadcasted_iota(jnp.int32, (n - rest, n), 1)
    kept = jnp.where((wide >= start) & (wide < rest), 0.0, work[rest:, :])
    work[rest:, :] = kept - update[rest - base :, :]


def solve_kernel(
    rows_total, gram_ref, y_big, y_small, out_hbm, work, inverse, out, store_sem,
):
    n = work.shape[0]
    half = n // 2
    blocks = gram_ref[...].astype(F32) * (1.0 / rows_total)
    work[:half, :half] = blocks[:half]
    work[half:, :half] = blocks[half : 2 * half]
    work[:half, half:] = blocks[half : 2 * half].T
    work[half:, half:] = blocks[2 * half :]
    for k in range(n // BLOCK):
        eliminate(work, inverse, k)
    factor = inverse[...]
    big = factor.astype(BF16)
    small = (factor - big.astype(F32)).astype(BF16)
    chunk = 256
    stores = []
    for i in range(y_big.shape[0] // chunk):
        span = pl.ds(i * chunk, chunk)
        out[span, :] = (
            dot(y_big[span, :], big, NT) + dot(y_big[span, :], small, NT) + dot(y_small[span, :], big, NT)
        )
        stores.append(pltpu.make_async_copy(out.at[span, :], out_hbm.at[span, :], store_sem.at[i]))
        stores[-1].start()
    for store in stores:
        store.wait()


def solved(rows_total, packed, y_big, y_small):
    rows, width = y_big.shape
    vmem = pl.BlockSpec(memory_space=pltpu.VMEM)
    return pl.pallas_call(
        functools.partial(solve_kernel, rows_total),
        out_shape=jax.ShapeDtypeStruct((rows, width), F32),
        in_specs=[vmem, vmem, vmem],
        out_specs=pl.BlockSpec(memory_space=pltpu.HBM),
        scratch_shapes=[
            pltpu.VMEM((width, width), F32),
            pltpu.VMEM((width, width), F32),
            pltpu.VMEM((rows, width), F32),
            pltpu.SemaphoreType.DMA((rows // 256,)),
        ],
        compiler_params=pltpu.CompilerParams(vmem_limit_bytes=24 * 1024 * 1024),
        name="solve",
    )(packed, y_big, y_small)


def on_device(sizes, tiles, tile_row, tile_col, tile_count, q_block):
    y_big, y_small, packed = summed_step(sizes, tiles, tile_row, tile_col, tile_count, q_block)
    rows_total = q_block.shape[0] * sizes[0] * sizes[1] * sizes[2] * sizes[3]
    return solved(rows_total, packed, y_big, y_small)


def solution(mesh):
    nz = mesh.shape["grp"]
    sizes = (nz, 8, mesh.shape["row"] // 16, 2)
    torus = Mesh(mesh.devices.reshape(sizes), AXES)
    return jax.shard_map(
        functools.partial(on_device, sizes),
        mesh=torus,
        in_specs=(P(AXES, None, None), P(AXES), P(AXES), P(AXES), P(AXES, None)),
        out_specs=P(AXES, None),
        check_vma=False,
    )
```
